32 devices in a mesh: blk: 8 (over z, y), plane: 4 (over x, core).
Axes of the slice: x: 2, y: 2, z: 4, core: 2. Of those that a mesh axis runs over, the one named last changes fastest.
Arguments:
- tiles: bfloat16 [128, 24, 128, 128], P(('blk', 'plane')), may hold values from -0.25 to 0.25
- tile_cols: int32 [128, 24], P(('blk', 'plane')), may hold values from 0 to 511
- tile_count: int32 [128], P(('blk', 'plane')), may hold values from 18 to 24, as said below
- u_start: float32 [16384], P(('blk', 'plane')), may hold values from -0.046875 to 0.046875
- v_start: float32 [65536], P(('blk', 'plane')), may hold values from -0.0234375 to 0.0234375
- beta_start: float32 [1], replicated, may hold values from 0.5 to 1.5
- left_basis: float32 [16384, 128], P(('blk', 'plane')), may hold values from -0.046875 to 0.046875
- right_basis: float32 [65536, 128], P(('blk', 'plane')), may hold values from -0.0234375 to 0.0234375
Outputs:
- left_vectors: float32 [1, 16384], P(None, ('blk', 'plane'))
- right_vectors: float32 [1, 65536], P(None, ('blk', 'plane'))
- coefficients: float32 [2], replicated
The draws below stay inside these ranges and needn't reach their ends.
Inputs may be any that keep to these rules, and one draw needn't show every extreme that they name: `tile_count`: slots at and after a row block's count are padding; some row block uses all 24 slots.
All inputs are finite; a program needn't handle non-finite values.
Results may differ from the reference program's by a relative error of at most 0.00055.
The reference program's roundings to bfloat16 on the way count: a program that leaves them out, or rounds other values in their place, can miss the bound.
Values may be sent and summed in bfloat16 or wider, within the bound.
A program may use at most 64 MiB of HBM per device.

```python
import jax
import jax.numpy as jnp
from jax import lax

N = 65536
NT = 512
SLOTS = 24
KB = 128
ITERS = 1
BLOCKS = 128
ROWS = 16384


def draw_tile_count(key, part):
    counts = jax.random.randint(key, (BLOCKS,), max(1, 3 * SLOTS // 4), SLOTS + 1).astype(jnp.int32)
    return counts.at[0].set(SLOTS)


def plant(drawn, own_key, smallest, top_value):
    dims = drawn.shape
    spot = [jax.random.randint(jax.random.fold_in(own_key, axis), (), 0, dims[axis]) for axis in range(len(dims))]
    drawn = drawn.at[tuple(spot)].set(smallest)
    longest = dims.index(max(dims))
    spot[longest] = (spot[longest] + 1) % dims[longest]
    return drawn.at[tuple(spot)].set(top_value)


def block_scale(stream_key, extent, cuts, low, largest):
    level, own = 1.0, jax.random.fold_in(stream_key, 6)
    for position, shards_of in cuts:
        draws = jnp.exp(jax.random.uniform(jax.random.fold_in(own, position), (shards_of,), jnp.float32, low / len(cuts), largest / len(cuts)))
        level = level * jnp.repeat(draws, extent[position] // shards_of).reshape([-1 if axis == position else 1 for axis in range(len(extent))])
    return level


def centred(rng, shape, spread, limit, shards=(), kind=jnp.bfloat16):
    drawn = spread * jax.random.normal(rng, shape, jnp.float32)
    if shards:
        drawn = drawn * block_scale(rng, shape, shards, -0.22, 0.18)
    return jnp.clip(drawn, -limit, limit).astype(kind)


def setup_inputs(seed: int = 0) -> dict:
    key_of = jax.random.split(jax.random.key(seed), 9)
    tiles = centred(key_of[0], (BLOCKS, SLOTS, 128, 128), (ROWS * SLOTS * 112 // N) ** -0.5, 0.25, ((0, 32),))
    tile_cols = plant(jax.random.randint(key_of[1], (BLOCKS, SLOTS), 0, NT), jax.random.fold_in(key_of[1], 1), 0, NT - 1).astype(jnp.int32)
    tile_count = draw_tile_count(jax.random.fold_in(key_of[8], 71), 0)
    u_start = centred(key_of[3], (ROWS,), ROWS ** -0.5, 0.046875, ((0, 32),), jnp.float32)
    v_start = centred(key_of[4], (N,), N ** -0.5, 0.0234375, ((0, 32),), jnp.float32)
    beta_start = jnp.clip(jax.random.uniform(key_of[5], (1,), jnp.float32, 0.5, 1.5), 0.5, 1.5)
    left_basis = centred(key_of[6], (ROWS, KB), ROWS ** -0.5, 0.046875, ((0, 32),), jnp.float32)
    right_basis = centred(key_of[7], (N, KB), N ** -0.5, 0.0234375, ((0, 32),), jnp.float32)
    return dict(tiles=tiles, tile_cols=tile_cols, tile_count=tile_count, u_start=u_start, v_start=v_start, beta_start=beta_start, left_basis=left_basis, right_basis=right_basis)


def project_twice(vec, basis):
    high = lax.Precision.HIGHEST
    first = jnp.dot(vec, basis, precision=high)
    vec = vec - jnp.dot(basis, first, precision=high)
    second = jnp.dot(vec, basis, precision=high)
    vec = vec - jnp.dot(basis, second, precision=high)
    norm = jnp.sqrt(jnp.sum(vec * vec) + 1e-06)
    return (vec / norm, norm)

def reference(tiles, tile_cols, tile_count, u_start, v_start, beta_start, left_basis, right_basis):
    high = lax.Precision.HIGHEST
    live = (jnp.arange(SLOTS, dtype=jnp.int32)[None, :] < tile_count[:, None]).astype(jnp.float32)

    def forward(rounded):
        table = rounded.reshape(-1, 128)

        def single(items):
            block, cols, weight = items
            picked = table[cols].astype(jnp.float32)
            values = jnp.einsum('sij,sj->si', block.astype(jnp.float32), picked, precision=high)
            return lax.optimization_barrier(jnp.sum(values * weight[:, None], axis=0))
        return lax.map(single, (tiles, tile_cols, live)).reshape(-1)

    def backward(rounded):
        table = rounded.reshape(-1, 128)

        def single(items):
            block, row, weight = items
            values = jnp.einsum('sij,i->sj', block.astype(jnp.float32), row.astype(jnp.float32), precision=high)
            return values * weight[:, None]
        contrib = lax.map(single, (tiles, table, live)).reshape(-1, 128)
        summed = jax.ops.segment_sum(contrib, tile_cols.reshape(-1), num_segments=N // 128)
        return summed.reshape(-1)
    vec_right = v_start
    vec_left = u_start
    beta = beta_start[0]
    lefts, rights, coefs = ([], [], [])
    for step in range(ITERS):
        forward_out = forward(vec_right.astype(jnp.bfloat16))
        vec_left, alpha = project_twice(forward_out - beta * vec_left, left_basis)
        back_out = backward(vec_left.astype(jnp.bfloat16))
        vec_right, beta = project_twice(back_out - alpha * vec_right, right_basis)
        lefts.append(vec_left * jnp.sqrt(jnp.float32(ROWS)))
        rights.append(vec_right * jnp.sqrt(jnp.float32(N)))
        coefs.append(alpha)
        coefs.append(beta)
    return (jnp.stack(lefts), jnp.stack(rights), jnp.stack(coefs))
```

```python
import functools
import math

import jax
import jax.numpy as jnp
from jax import lax
from jax.experimental import pallas as pl
from jax.experimental.pallas import tpu as pltpu
from jax.sharding import PartitionSpec as P

AXES = ("blk", "plane")
HIGH = lax.Precision.HIGHEST
LANES = 128
NT_DIMS = (((1,), (1,)), ((), ()))


def steps_kernel(
    devices,
    planes,
    own_tiles,
    left_scale,
    right_scale,
    beta_ref,
    count_ref,
    cols_ref,
    u_ref,
    v_ref,
    tiles_hbm,
    left_hbm,
    right_hbm,
    out_left,
    out_right,
    out_coef,
    tiles,
    left,
    right,
    left_t,
    right_t,
    v_send,
    v_all,
    cols_rows,
    pick_hot,
    put_hot,
    picked,
    contrib,
    gram_send,
    gram_recv,
    gram_sum,
    gram_all,
    dot_send,
    dot_recv,
    part_send,
    part_recv,
    own_scr,
    p_scr,
    copy_sem,
    send_sem,
    recv_sem,
):
    blocks, slots = cols_ref.shape
    keep = left.shape[1]
    me_blk, me_plane = lax.axis_index("blk"), lax.axis_index("plane")
    me = me_blk * planes + me_plane
    chunks = gram_send.shape[0]
    pad_tiles = v_send.shape[0]
    part_rows = part_send.shape[1]
    stride = picked.shape[0] // blocks

    def target(step):
        other = lax.rem(me + step, devices)
        return other, (other // planes, lax.rem(other, planes))

    barrier = pltpu.get_barrier_semaphore()

    def greet(step, carry):
        _, place = target(step)
        pl.semaphore_signal(
            barrier, inc=1, device_id=place, device_id_type=pl.DeviceIdType.MESH
        )
        return carry

    lax.fori_loop(1, devices, greet, 0)

    loads = [
        pltpu.make_async_copy(left_hbm, left, copy_sem.at[0]),
        pltpu.make_async_copy(right_hbm, right, copy_sem.at[1]),
        pltpu.make_async_copy(tiles_hbm, tiles, copy_sem.at[2]),
    ]
    for load in loads:
        load.start()

    def send_all(phase, source, landing):
        def body(step, carry):
            other, place = target(step)
            pltpu.make_async_remote_copy(
                src_ref=source(other),
                dst_ref=landing.at[me],
                send_sem=send_sem.at[phase],
                recv_sem=recv_sem.at[phase],
                device_id=place,
                device_id_type=pl.DeviceIdType.MESH,
            ).start()
            return carry

        lax.fori_loop(1, devices, body, 0)

    def wait_all(sem, phase, landing):
        most = landing.at[pl.ds(0, devices - 1)]
        pltpu.make_async_copy(most, most, sem.at[phase]).wait()

    eye = lax.broadcasted_iota(jnp.int32, (LANES, LANES), 0) == lax.broadcasted_iota(
        jnp.int32, (LANES, LANES), 1
    )

    def to_col(row):
        return jnp.sum(jnp.where(eye, row, 0.0), axis=1, keepdims=True)

    def to_row(col):
        return jnp.sum(jnp.where(eye, col, 0.0), axis=0, keepdims=True)

    rounded = v_ref[...].astype(jnp.bfloat16)
    if pad_tiles > own_tiles:
        rounded = jnp.concatenate(
            [v_ref[...], jnp.zeros((pad_tiles - own_tiles, LANES), jnp.float32)], axis=0
        ).astype(jnp.bfloat16)
    v_send[...] = rounded
    v_all[me] = rounded
    pl.semaphore_wait(barrier, devices - 1)
    send_all(0, lambda other: v_send, v_all)

    loads[0].wait()
    loads[1].wait()
    for r in range(left.shape[0] // LANES):
        left_t[:, r * LANES : (r + 1) * LANES] = left[r * LANES : (r + 1) * LANES, :].T
    for t in range(own_tiles):
        right_t[:, t * LANES : (t + 1) * LANES] = right[t * LANES : (t + 1) * LANES, :].T
    rows = gram_send.shape[1]
    half = keep // rows
    gram = lax.dot_general(
        left_t[...], left_t[...], NT_DIMS, precision=HIGH, preferred_element_type=jnp.float32
    )
    gram_send[0:half] = gram.reshape(half, rows, keep)
    gram = lax.dot_general(
        right_t[...], right_t[...], NT_DIMS, precision=HIGH, preferred_element_type=jnp.float32
    )
    gram_send[half : 2 * half] = gram.reshape(half, rows, keep)
    gram_recv[me] = gram_send[lax.rem(me, chunks)]
    send_all(1, lambda other: gram_send.at[lax.rem(other, chunks)], gram_recv)

    cols_rows[...] = jnp.full(cols_rows.shape, -1.0, jnp.float32)
    for r in range(blocks):
        row = cols_ref[r : r + 1, :]
        alive = lax.broadcasted_iota(jnp.int32, (1, slots), 1) < count_ref[r]
        cols_rows[r : r + 1, 0:slots] = jnp.where(alive, row, -1).astype(jnp.float32)
    entries = picked.shape[0]
    lane = lax.broadcasted_iota(jnp.int32, (1, entries), 1)
    line = jnp.full((1, entries), -1.0, jnp.float32)
    for r in range(blocks):
        row = cols_rows[r : r + 1, :]
        if r:
            row = pltpu.roll(row, r * stride, 1)
        line = jnp.where((lane >= r * stride) & (lane < r * stride + slots), row, line)
    whole = line.astype(jnp.int32)
    pick_row = jnp.where(whole < 0, -1, whole // own_tiles * pad_tiles + whole % own_tiles)
    put_row = jnp.where(whole < 0, -1, whole // own_tiles * part_rows + whole % own_tiles)
    pick_col = to_col(pick_row.astype(jnp.float32)).astype(jnp.int32)
    pick_hot[...] = jnp.where(
        lax.broadcasted_iota(jnp.int32, pick_hot.shape, 1) == pick_col, 1.0, 0.0
    ).astype(jnp.bfloat16)
    put_hot[...] = jnp.where(
        lax.broadcasted_iota(jnp.int32, put_hot.shape, 0) == put_row, 1.0, 0.0
    ).astype(jnp.bfloat16)
    contrib[...] = jnp.zeros_like(contrib)

    wait_all(recv_sem, 0, v_all)
    picked[...] = jnp.dot(
        pick_hot[...],
        v_all[...].reshape(devices * pad_tiles, LANES),
        preferred_element_type=jnp.float32,
    )
    loads[2].wait()
    beta = beta_ref[0]

    def forward(r, carry):
        total = jnp.zeros((LANES, LANES), jnp.float32)
        for s in range(slots):
            total = total + tiles[r, s].astype(jnp.float32) * picked[pl.ds(r * stride + s, 1), :]
        q = to_row(jnp.sum(total, axis=1, keepdims=True))
        p_scr[pl.ds(r, 1), :] = q - beta * u_ref[pl.ds(r, 1), :]
        return carry

    lax.fori_loop(0, blocks, forward, 0)

    def start_dots(phase, basis_t, vec, count):
        total = jnp.zeros((keep, LANES), jnp.float32)
        for r in range(count):
            total = total + basis_t[:, r * LANES : (r + 1) * LANES] * vec[r : r + 1, :]
        dots = to_row(jnp.sum(total, axis=1, keepdims=True))
        square = jnp.sum(vec * vec, keepdims=True)
        both = jnp.concatenate([dots, jnp.broadcast_to(square, (1, LANES))], axis=0)
        side = phase // 4
        dot_send[side] = both
        dot_recv[side, me] = both
        send_all(phase, lambda other: dot_send.at[side], dot_recv.at[side])

    def finish_dots(phase, gram):
        side = phase // 4
        wait_all(recv_sem, phase, dot_recv.at[side])
        both = jnp.sum(dot_recv[side], axis=0)
        first, square = both[0:1, :], both[1:2, 0:1]
        coef = 2.0 * to_col(first) - jnp.sum(gram * first, axis=1, keepdims=True)
        coef_row = to_row(coef)
        spread = jnp.sum(gram * coef_row, axis=1, keepdims=True)
        total = (
            square
            - 2.0 * jnp.sum(coef_row * first, keepdims=True)
            + jnp.sum(coef * spread, keepdims=True)
        )
        return coef, jnp.sqrt(total + 1e-06)

    p = p_scr[0:blocks, :]
    start_dots(3, left_t, p, blocks)

    wait_all(recv_sem, 1, gram_recv)
    mine = jnp.sum(gram_recv[...], axis=0)
    gram_sum[...] = mine
    gram_all[me] = mine
    send_all(2, lambda other: gram_sum, gram_all)
    wait_all(recv_sem, 2, gram_all)

    coef, alpha = finish_dots(3, gram_all[0:half].reshape(keep, keep))
    out_coef[0] = alpha[0, 0]
    for r in range(blocks):
        fix = jnp.sum(left_t[:, r * LANES : (r + 1) * LANES] * coef, axis=0, keepdims=True)
        p_scr[r : r + 1, :] = (p[r : r + 1, :] - fix) / alpha
    out_left[...] = p_scr[0:blocks, :] * left_scale

    def backward(r, carry):
        row = p_scr[pl.ds(r, 1), :].astype(jnp.bfloat16).astype(jnp.float32)
        col = jnp.broadcast_to(to_col(row), (LANES, LANES))
        for g in range(0, slots, 8):
            lines = [
                jnp.sum(tiles[r, s].astype(jnp.float32) * col, axis=0, keepdims=True)
                for s in range(g, min(g + 8, slots))
            ]
            contrib[pl.ds(pl.multiple_of(r * stride + g, 8), len(lines)), :] = jnp.concatenate(
                lines, axis=0
            )
        return carry

    lax.fori_loop(0, blocks, backward, 0)
    rest = contrib[...]
    spread = jnp.zeros((devices * part_rows, LANES), jnp.float32)
    for _ in range(3):
        piece = rest.astype(jnp.bfloat16)
        rest = rest - piece.astype(jnp.float32)
        spread = spread + jnp.dot(put_hot[...], piece, preferred_element_type=jnp.float32)
    part_send[...] = spread.reshape(devices, part_rows, LANES)
    part_recv[me] = part_send[me]
    send_all(5, lambda other: part_send.at[other], part_recv)
    wait_all(recv_sem, 5, part_recv)
    own_scr[...] = jnp.sum(part_recv[...], axis=0)
    r_vec = own_scr[0:own_tiles, :] - alpha * v_ref[...]
    start_dots(4, right_t, r_vec, own_tiles)
    coef, beta_new = finish_dots(4, gram_all[half : 2 * half].reshape(keep, keep))
    out_coef[1] = beta_new[0, 0]
    for t in range(own_tiles):
        fix = jnp.sum(right_t[:, t * LANES : (t + 1) * LANES] * coef, axis=0, keepdims=True)
        out_right[t : t + 1, :] = (r_vec[t : t + 1, :] - fix) / beta_new * right_scale

    wait_all(send_sem, 0, v_all)
    wait_all(send_sem, 1, gram_recv)
    wait_all(send_sem, 2, gram_all)
    wait_all(send_sem, 3, dot_recv.at[0])
    wait_all(send_sem, 4, dot_recv.at[1])
    wait_all(send_sem, 5, part_recv)


def on_device(tiles, tile_cols, tile_count, u_start, v_start, beta_start, left_basis, right_basis):
    devices = lax.axis_size(AXES)
    planes = lax.axis_size("plane")
    blocks, slots = tile_cols.shape
    own_tiles = v_start.shape[0] // LANES
    left_rows, keep = left_basis.shape
    right_rows = right_basis.shape[0]
    pad_tiles = -(-own_tiles // 16) * 16
    part_rows = -(-own_tiles // 8) * 8
    rows = max(8, 2 * keep // devices)
    chunks = 2 * keep // rows
    stride = -(-slots // 8) * 8
    while (blocks * stride) % LANES:
        stride += 8
    entries = blocks * stride
    f32, bf16 = jnp.float32, jnp.bfloat16
    vmem = pl.BlockSpec(memory_space=pltpu.VMEM)
    smem = pl.BlockSpec(memory_space=pltpu.SMEM)
    hbm = pl.BlockSpec(memory_space=pl.ANY)
    left_out, right_out, coefs = pl.pallas_call(
        functools.partial(
            steps_kernel,
            devices,
            planes,
            own_tiles,
            math.sqrt(left_rows * devices),
            math.sqrt(right_rows * devices),
        ),
        out_shape=(
            jax.ShapeDtypeStruct((blocks, LANES), f32),
            jax.ShapeDtypeStruct((own_tiles, LANES), f32),
            jax.ShapeDtypeStruct((2,), f32),
        ),
        in_specs=[smem, smem, vmem, vmem, vmem, hbm, hbm, hbm],
        out_specs=(vmem, vmem, smem),
        scratch_shapes=[
            pltpu.VMEM(tiles.shape, bf16),
            pltpu.VMEM(left_basis.shape, f32),
            pltpu.VMEM(right_basis.shape, f32),
            pltpu.VMEM((keep, left_rows), f32),
            pltpu.VMEM((keep, right_rows), f32),
            pltpu.VMEM((pad_tiles, LANES), bf16),
            pltpu.VMEM((devices, pad_tiles, LANES), bf16),
            pltpu.VMEM((-(-blocks // 8) * 8, entries), f32),
            pltpu.VMEM((entries, devices * pad_tiles), bf16),
            pltpu.VMEM((devices * part_rows, entries), bf16),
            pltpu.VMEM((entries, LANES), f32),
            pltpu.VMEM((entries, LANES), f32),
            pltpu.VMEM((chunks, rows, keep), f32),
            pltpu.VMEM((devices, rows, keep), f32),
            pltpu.VMEM((rows, keep), f32),
            pltpu.VMEM((devices, rows, keep), f32),
            pltpu.VMEM((2, 2, keep), f32),
            pltpu.VMEM((2, devices, 2, keep), f32),
            pltpu.VMEM((devices, part_rows, LANES), f32),
            pltpu.VMEM((devices, part_rows, LANES), f32),
            pltpu.VMEM((part_rows, LANES), f32),
            pltpu.VMEM((-(-blocks // 8) * 8, LANES), f32),
            pltpu.SemaphoreType.DMA((3,)),
            pltpu.SemaphoreType.DMA((6,)),
            pltpu.SemaphoreType.DMA((6,)),
        ],
        compiler_params=pltpu.CompilerParams(
            collective_id=0, has_side_effects=True, vmem_limit_bytes=60 * 1024 * 1024
        ),
    )(
        beta_start,
        tile_count,
        tile_cols,
        u_start.reshape(blocks, LANES),
        v_start.reshape(own_tiles, LANES),
        tiles,
        left_basis,
        right_basis,
    )
    return left_out.reshape(1, -1), right_out.reshape(1, -1), coefs


def solution(mesh):
    placed = (
        P(AXES, None, None, None),
        P(AXES, None),
        P(AXES),
        P(AXES),
        P(AXES),
        P(),
        P(AXES, None),
        P(AXES, None),
    )
    return jax.shard_map(
        on_device,
        mesh=mesh,
        in_specs=placed,
        out_specs=(P(None, AXES), P(None, AXES), P()),
        check_vma=False,
    )
```
